32 devices in a mesh: rep: 8 (over z, x), tp: 4 (over y, core).
Axes of the slice: x: 2, y: 2, z: 4, core: 2. Of those that a mesh axis runs over, the one named last changes fastest.
Arguments:
- stream_in: bfloat16 [32, 4, 8192], P('rep', None, 'tp'), may hold values from -6 to 6
- queries: bfloat16 [32, 4, 4096], P('rep'), may hold values from -90 to 90
- new_keys: bfloat16 [32, 4, 4, 128], P('rep'), may hold values from -4 to 4
- new_values: bfloat16 [32, 4, 4, 128], P('rep'), may hold values from -4 to 4
- key_cache: bfloat16 [32, 1024, 4, 128], P('rep', 'tp'), may hold values from -4.1 to 4.1
- value_cache: bfloat16 [32, 1024, 4, 128], P('rep', 'tp'), may hold values from -4 to 4
- lengths: int32 [32], P('rep'), may hold values from 2 to 1024
- out_weight: bfloat16 [4096, 8192], P('tp', 'rep'), may hold values from -0.09375 to 0.09375
- norm_gain: bfloat16 [8192], P('tp'), may hold values from 0.5 to 1.5
Outputs:
- stream_out: bfloat16 [32, 4, 8192], P('rep', None, 'tp')
- normed: bfloat16 [32, 4, 8192], P('rep', None, 'tp')
The draws below stay inside these ranges and needn't reach their ends.
All inputs are finite; a program needn't handle non-finite values.
Results may differ from the reference program's by a relative error of at most 0.0065.
Values may be sent and summed in bfloat16 or wider, within the bound.
A program may use at most 64 MiB of HBM per device.

```python
import math
import jax
import jax.numpy as jnp
from jax import lax

D = 8192
HEADS = 32
KV_HEADS = 4
HD = 128
STEPS = 4
ROWS = 32
CTX = 1024
FEAT = 4096
N_TP = 4


def shared_keys(key):
    base = jax.random.normal(jax.random.fold_in(key, 11), (ROWS, CTX, KV_HEADS, HD), jnp.float32)
    base = jnp.clip(base, -4.0, 4.0)
    return base


def draw_key_cache(key, part):
    return shared_keys(key).astype(jnp.bfloat16)


def draw_queries(key, part):
    drawn = jax.random.normal(jax.random.fold_in(key, 23), (ROWS, STEPS, HEADS * HD), jnp.float32)
    drawn = jnp.clip(drawn, -4.0, 4.0)
    return drawn.astype(jnp.bfloat16)


def plant(values, stream_key, least, top_value):
    longest = values.shape.index(max(values.shape))
    spots = []
    for shift in (0, 1):
        where = [jax.random.randint(jax.random.fold_in(stream_key, axis), (), 0, length) for axis, length in enumerate(values.shape)]
        where[longest] = (where[longest] + shift) % values.shape[longest]
        spots.append(tuple(where))
    return values.at[spots[0]].set(least).at[spots[1]].set(top_value)


def levels(own_key, dims, cuts, low, largest):
    loudness = 1.0
    for position, parts in cuts:
        heights = jax.random.uniform(jax.random.fold_in(jax.random.fold_in(own_key, 6), position), (parts,), jnp.float32, low / len(cuts), largest / len(cuts))
        loudness = loudness * jnp.repeat(jnp.exp(heights), dims[position] // parts).reshape((-1,) + (1,) * (len(dims) - 1 - position))
    return loudness


def centred(own_key, extent, width, bound, shards=(), kind=jnp.bfloat16):
    result = jax.random.normal(own_key, extent, jnp.float32) * width
    if len(shards) > 0:
        result = levels(own_key, extent, shards, -0.22, 0.18) * result
    return jnp.clip(result, min=-bound, max=bound).astype(kind)


def setup_inputs(seed: int = 0) -> dict:
    key_list = jax.random.split(jax.random.key(seed), 10)
    return {
        "stream_in": centred(key_list[0], (ROWS, STEPS, D), 1.0, 6.0, ((0, 8), (2, 4))),
        "queries": draw_queries(jax.random.fold_in(key_list[9], 71), 0),
        "new_keys": centred(key_list[2], (ROWS, STEPS, KV_HEADS, HD), 1.0, 4.0, ((0, 8),)),
        "new_values": centred(key_list[3], (ROWS, STEPS, KV_HEADS, HD), 1.0, 4.0, ((0, 8),)),
        "key_cache": draw_key_cache(jax.random.fold_in(key_list[9], 71), 0),
        "value_cache": centred(key_list[5], (ROWS, CTX, KV_HEADS, HD), 1.0, 4.0, ((0, 8), (1, 4))),
        "lengths": plant(jax.random.randint(key_list[6], (ROWS,), 2, CTX + 1), jax.random.fold_in(key_list[6], 1), 2, CTX).astype(jnp.int32),
        "out_weight": centred(key_list[7], (FEAT, D), FEAT ** -0.5, 0.09375, ((0, 4), (1, 8))),
        "norm_gain": jnp.clip(1.0 + 0.1 * jax.random.normal(key_list[8], (D,), jnp.float32), 0.5, 1.5).astype(jnp.bfloat16),
    }


def attend_row(packed):
    query, key_new, value_new, key_old, value_old, length = packed
    group_size = HEADS // KV_HEADS
    scaling = 1.0 / math.sqrt(HD)
    query_f = query.astype(jnp.float32).reshape(STEPS, KV_HEADS, group_size, HD)
    cached = jnp.einsum('sgjd,pgd->sgjp', query_f, key_old.astype(jnp.float32)) * scaling
    visible = jnp.arange(CTX) < length
    cached = jnp.where(visible[None, None, None, :], cached, -1e+30)
    fresh = jnp.einsum('sgjd,tgd->sgjt', query_f, key_new.astype(jnp.float32)) * scaling
    causal = jnp.arange(STEPS)[None, :] <= jnp.arange(STEPS)[:, None]
    fresh = jnp.where(causal[:, None, None, :], fresh, -1e+30)
    maxima = jnp.maximum(cached.max(-1), fresh.max(-1))
    weights_cached = jnp.exp(cached - maxima[..., None])
    weights_fresh = jnp.exp(fresh - maxima[..., None])
    denominator = weights_cached.sum(-1) + weights_fresh.sum(-1)
    rounded_cached = lax.optimization_barrier(weights_cached.astype(jnp.bfloat16)).astype(jnp.float32)
    rounded_fresh = lax.optimization_barrier(weights_fresh.astype(jnp.bfloat16)).astype(jnp.float32)
    numerator = jnp.einsum('sgjp,pgd->sgjd', rounded_cached, value_old.astype(jnp.float32))
    numerator = numerator + jnp.einsum('sgjt,tgd->sgjd', rounded_fresh, value_new.astype(jnp.float32))
    attended = (numerator / denominator[..., None]).astype(jnp.bfloat16)
    return attended.reshape(STEPS, HEADS * HD)

def reference(stream_in, queries, new_keys, new_values, key_cache, value_cache, lengths, out_weight, norm_gain):
    attended = lax.map(attend_row, (queries, new_keys, new_values, key_cache, value_cache, lengths))
    flat = attended.reshape(ROWS * STEPS, HEADS * HD)
    width_share = HEADS * HD // N_TP
    summed = jnp.zeros((ROWS * STEPS, D), jnp.float32)
    for group_index in range(N_TP):
        lower = group_index * width_share
        partial_value = jnp.dot(flat[:, lower:lower + width_share], out_weight[lower:lower + width_share], preferred_element_type=jnp.float32)
        summed = summed + lax.optimization_barrier(partial_value.astype(jnp.bfloat16)).astype(jnp.float32)
    hidden = stream_in.reshape(ROWS * STEPS, D).astype(jnp.float32) + summed
    inverse = lax.rsqrt(lax.optimization_barrier(jnp.mean(hidden * hidden, axis=1)) + 1e-06)
    normed = hidden * inverse[:, None] * norm_gain.astype(jnp.float32)[None, :]
    stream_out = hidden.astype(jnp.bfloat16).reshape(ROWS, STEPS, D)
    return (stream_out, normed.astype(jnp.bfloat16).reshape(ROWS, STEPS, D))
```

```python
import functools
import math

import jax
import jax.numpy as jnp
from jax import lax
from jax.experimental import pallas as pl
from jax.experimental.pallas import tpu as pltpu
from jax.sharding import PartitionSpec as P

MESH = pl.DeviceIdType.MESH
PAD = 128
LANES = 128
TILE = 8
LOADS = 5
SINGLES = 10


def flip(index, mask, count):
    other = 0
    bit = 1
    while bit < count:
        digit = (index // bit) % 2
        other = other + bit * ((1 - digit) if mask & bit else digit)
        bit *= 2
    return other


def landed(ref, sem):
    pltpu.make_async_copy(ref, ref, sem).wait()


def attend(cfg, b, length, tp, q_v, kv_v):
    n_rep, n_tp, batch, steps, heads, kv, block_len, width_all, eps = cfg
    hd = q_v.shape[2]
    group = steps * (heads // kv)
    cached = block_len * kv
    fresh = steps * kv
    chunks = cached // LANES
    scaling = 1.0 / math.sqrt(hd)
    lane = lax.broadcasted_iota(jnp.int32, (group, LANES), 1)
    row = lax.broadcasted_iota(jnp.int32, (group, LANES), 0)
    kind = lane % kv
    place = lane // kv
    causal = (place <= row % steps) & (lane < fresh) & (tp == 0)
    s = lax.dot_general(
        q_v[b], kv_v[b, 0], (((1,), (1,)), ((), ())), preferred_element_type=jnp.float32
    )
    left = length - tp * block_len
    kept = []
    for c in range(chunks + 1):
        own = s[0:group, c * LANES : (c + 1) * LANES]
        for g in range(1, kv):
            own = jnp.where(kind == g, s[g * group : (g + 1) * group, c * LANES : (c + 1) * LANES], own)
        seen = place < left - c * (LANES // kv) if c < chunks else causal
        kept.append(jnp.where(seen, own, -1e30))
    highest = functools.reduce(jnp.maximum, kept)
    tops = [jnp.max(jnp.where(kind == g, highest, -3e38), axis=1, keepdims=True) for g in range(kv)]
    top = jnp.broadcast_to(tops[0], (group, LANES))
    for g in range(1, kv):
        top = jnp.where(kind == g, tops[g], top)
    weights = [jnp.exp((k - top) * scaling) for k in kept]
    summed = functools.reduce(jnp.add, weights)
    totals = [jnp.sum(jnp.where(kind == g, summed, 0.0), axis=1, keepdims=True) for g in range(kv)]
    rounded = jnp.concatenate([w.astype(jnp.bfloat16) for w in weights], axis=1)
    one = jnp.where(kind == 0, 1.0, 0.0)
    spread = []
    for g in range(kv):
        one = jnp.where(kind == g, 1.0, 0.0).astype(jnp.bfloat16)
        spread.append(rounded * jnp.concatenate([one] * (chunks + 1), axis=1))
    spread = jnp.concatenate(spread, axis=0)
    num = jnp.dot(spread, kv_v[b, 1], preferred_element_type=jnp.float32)
    total = jnp.concatenate(totals, axis=0)
    return (num / total).astype(jnp.bfloat16), jnp.concatenate(tops, axis=0) * scaling + jnp.log(total)


def kernel(
    cfg, order, far,
    len_hbm, q_hbm, nk_hbm, nv_hbm, k_hbm, v_hbm, w_hbm, x_hbm, gain_hbm,
    hidden_ref, scale_ref,
    len_s, q_v, kv_v, w_v, gain_v,
    send_o, recv_o, send_l, recv_l, mix,
    gathered, parts, other, ready, recv_c, x_v, sq_s, sq_r,
    sems,
):
    n_rep, n_tp, batch, steps, heads, kv, block_len, width_all, eps = cfg
    rep = lax.axis_index("rep")
    tp = lax.axis_index("tp")
    k_own = n_rep // n_tp
    pairs = n_rep // 2
    rows = batch * steps
    owned = heads // n_tp
    orow = owned * steps
    hs = heads * steps
    cached = block_len * kv
    fresh = steps * kv
    cw = w_v.shape[1]
    hd = q_v.shape[2]
    owner = rep // k_own
    core = lax.rem(tp, 2)
    chips = n_tp // 2
    is_own = (owner == tp) & (lax.rem(rep, 2) == core)
    not_own = jnp.logical_not(is_own)
    slot = lax.rem(rep, k_own) * chips + tp // 2

    s_len, s_q, s_w, s_gain, s_x = (sems.at[i] for i in range(LOADS))
    s_kv = [sems.at[LOADS + b] for b in range(batch)]
    first = LOADS + batch
    (ao_s, ao_r, al_s, al_r, b_s, d_s, c_s, c_r, q_s, q_r) = (
        sems.at[first + i] for i in range(SINGLES)
    )
    first += SINGLES
    b_r = [sems.at[first + p] for p in range(pairs)]
    d_r = [sems.at[first + pairs + p] for p in range(pairs)]

    loads = [pltpu.make_async_copy(q_hbm, q_v, s_q)]
    for b in range(batch):
        loads += [
            pltpu.make_async_copy(k_hbm.at[b], kv_v.at[b, 0, pl.ds(0, cached)], s_kv[b]),
            pltpu.make_async_copy(nk_hbm.at[b], kv_v.at[b, 0, pl.ds(cached, fresh)], s_kv[b]),
            pltpu.make_async_copy(v_hbm.at[b], kv_v.at[b, 1, pl.ds(0, cached)], s_kv[b]),
            pltpu.make_async_copy(nv_hbm.at[b], kv_v.at[b, 1, pl.ds(cached, fresh)], s_kv[b]),
        ]
        if b == 0:
            loads.append(pltpu.make_async_copy(len_hbm, len_s, s_len))
    loads += [
        pltpu.make_async_copy(w_hbm, w_v, s_w),
        pltpu.make_async_copy(gain_hbm, gain_v, s_gain),
        pltpu.make_async_copy(x_hbm, x_v, s_x),
    ]
    for c in loads:
        c.start()

    barrier = pltpu.get_barrier_semaphore()
    for j in range(n_rep - 1, 0, -1):
        pl.semaphore_signal(barrier, inc=1, device_id=(lax.rem(rep + j, n_rep), tp), device_id_type=MESH)
    for j in range(1, n_tp):
        pl.semaphore_signal(barrier, inc=1, device_id=(rep, lax.rem(tp + j, n_tp)), device_id_type=MESH)
    for i in range(k_own):
        for h in range(chips):
            source = (tp * k_own + i, 2 * h + lax.rem(rep, 2))
            mine = (source[0] == rep) & (source[1] == tp)

            @pl.when(jnp.logical_not(mine))
            def _():
                pl.semaphore_signal(barrier, inc=1, device_id=source, device_id_type=MESH)

    for b in range(batch):
        for i in range(2):
            kv_v[b, i, cached + fresh : cached + PAD, :] = jnp.zeros((PAD - fresh, hd), jnp.bfloat16)

    lane = lax.broadcasted_iota(jnp.int32, (hs, LANES), 1)
    lse = jnp.zeros((hs, LANES), jnp.float32)
    landed(len_s, s_len)
    landed(q_v, s_q)
    together = 2 if batch % 2 == 0 else 1
    for b0 in range(0, batch, together):
        for b in range(b0, b0 + together):
            landed(kv_v.at[b, :, pl.ds(0, cached + fresh)], s_kv[b])
        for b in range(b0, b0 + together):
            out, value = attend(cfg, b, len_s[b], tp, q_v, kv_v)
            for t in range(n_tp):
                send_o[t, b] = out[t * orow : (t + 1) * orow]
            lse = jnp.where(lane == b, value, lse)
    send_l[...] = lse.T[:TILE]

    pl.semaphore_wait(barrier, (n_tp - 1) + (n_rep - 1) + n_rep // 2 - is_own.astype(jnp.int32))
    for j in range(1, n_tp):
        peer = lax.rem(tp + j, n_tp)
        pltpu.make_async_remote_copy(
            send_l, recv_l.at[j - 1], al_s, al_r, device_id=(rep, peer), device_id_type=MESH).start()
        pltpu.make_async_remote_copy(
            send_o.at[peer], recv_o.at[j - 1], ao_s, ao_r, device_id=(rep, peer), device_id_type=MESH).start()

    landed(recv_l, al_r)
    ls = [send_l[...]] + [recv_l[j] for j in range(n_tp - 1)]
    most = functools.reduce(jnp.maximum, ls)
    ws = [jnp.exp(l - most) for l in ls]
    inv = 1.0 / functools.reduce(jnp.add, ws)
    ws = [w * inv for w in ws]
    if n_tp * TILE < LANES:
        ws.append(jnp.zeros((LANES - n_tp * TILE, hs), jnp.float32))
    mix[...] = jnp.concatenate(ws, axis=0).T
    share = mix[pl.ds(pl.multiple_of(tp * orow, orow), orow), :]
    landed(recv_o, ao_r)
    att = []
    for b in range(batch):
        acc = share[:, b : b + 1] * send_o[tp, b].astype(jnp.float32)
        for j in range(1, n_tp):
            acc = acc + share[:, j * TILE + b : j * TILE + b + 1] * recv_o[j - 1, b].astype(jnp.float32)
        att.append(acc.astype(jnp.bfloat16))
    att = jnp.concatenate(att, axis=0)
    m = batch * orow
    to = lax.broadcasted_iota(jnp.int32, (m, m), 0)
    frm = lax.broadcasted_iota(jnp.int32, (m, m), 1)
    want = ((to // steps) % batch) * orow + (to // rows) * steps + to % steps
    pick = jnp.where(frm == want, 1.0, 0.0).astype(jnp.bfloat16)
    att = jnp.dot(pick, att, preferred_element_type=jnp.float32).astype(jnp.bfloat16)
    gathered[rep] = jnp.concatenate([att[h * rows : (h + 1) * rows] for h in range(owned)], axis=1)

    for mask in far:
        pltpu.make_async_remote_copy(
            gathered.at[rep], gathered.at[rep], b_s, sems.at[first + rep // 2],
            device_id=(flip(rep, mask, n_rep), tp), device_id_type=MESH).start()
    partner = tp + 1 - 2 * core

    def pass_on(p):
        landed(other.at[p], d_r[p])
        both = parts[p, core].astype(jnp.float32) + other[p].astype(jnp.float32)
        ready[p] = both.astype(jnp.bfloat16)
        local = is_own & (rep // 2 == p)

        @pl.when(jnp.logical_not(local))
        def _():
            pltpu.make_async_remote_copy(
                ready.at[p], recv_c.at[slot], c_s, c_r,
                device_id=(2 * p + core, owner), device_id_type=MESH).start()

        @pl.when(local)
        def _():
            recv_c[slot] = ready[p]

    landed(w_v, s_w)
    waiting = []
    for batch_of in order:
        for p in batch_of:
            mine = rep // 2 == p

            @pl.when(mine)
            def _():
                landed(gathered.at[0], b_r[p])

            @pl.when(jnp.logical_not(mine))
            def _():
                landed(gathered.at[pl.ds(2 * p, 2)], b_r[p])

        block = jnp.concatenate([gathered[2 * p + i] for p in batch_of for i in range(2)], axis=0)
        proj = jnp.dot(block, w_v[...], preferred_element_type=jnp.float32).astype(jnp.bfloat16)
        for n, p in enumerate(batch_of):
            for i in range(2):
                parts[p, i] = proj[(2 * n + i) * rows : (2 * n + i + 1) * rows]
            pltpu.make_async_remote_copy(
                parts.at[p, 1 - core], other.at[p], d_s, d_r[p],
                device_id=(rep, partner), device_id_type=MESH).start()
        for p in waiting:
            pass_on(p)
        waiting = batch_of
    for p in waiting:
        pass_on(p)

    landed(x_v, s_x)
    landed(gain_v, s_gain)
    gain = gain_v[...].astype(jnp.float32)
    gain = jnp.concatenate([gain[c : c + 1] for c in range(gain.shape[0])], axis=1)

    x = x_v[...].astype(jnp.float32).reshape(rows, x_v.shape[2])
    spot = lax.broadcasted_iota(jnp.int32, (rows, LANES), 0) == lax.broadcasted_iota(jnp.int32, (rows, LANES), 1)

    @pl.when(is_own)
    def _():
        landed(recv_c.at[pl.ds(0, n_rep // 2 - 1)], c_r)

    @pl.when(not_own)
    def _():
        landed(recv_c, c_r)

    pieces = []
    for i in range(k_own):
        acc = recv_c[i * chips].astype(jnp.float32)
        for h in range(1, chips):
            acc = acc + recv_c[i * chips + h].astype(jnp.float32)
        pieces.append(acc)
    hidden = x + jnp.concatenate(pieces, axis=1)
    squares = jnp.sum(hidden * hidden, axis=1, keepdims=True)
    sq_s[...] = jnp.sum(jnp.where(spot, squares, 0.0), axis=0, keepdims=True)
    for j in range(1, n_tp):
        pltpu.make_async_remote_copy(
            sq_s, sq_r.at[pl.ds(j, 1)], q_s, q_r,
            device_id=(rep, lax.rem(tp + j, n_tp)), device_id_type=MESH).start()
    sq_r[0:1, :] = sq_s[...]
    hidden_ref[...] = hidden.reshape(hidden_ref.shape)
    landed(sq_r.at[pl.ds(1, n_tp - 1)], q_r)
    every = jnp.sum(sq_r[...], axis=0, keepdims=True)
    every = jnp.sum(jnp.where(spot, every, 0.0), axis=1, keepdims=True)
    inverse = lax.rsqrt(every / width_all + eps)
    scale_ref[...] = (inverse * gain).reshape(scale_ref.shape)

    landed(recv_l, al_s)
    landed(recv_o, ao_s)
    landed(gathered.at[pl.ds(1, n_rep - 1)], b_s)
    landed(other, d_s)
    landed(sq_r.at[pl.ds(1, n_tp - 1)], q_s)

    @pl.when(is_own)
    def _():
        landed(ready.at[pl.ds(0, pairs - 1)], c_s)

    @pl.when(not_own)
    def _():
        landed(ready, c_s)


def on_device(
    n_rep, n_tp,
    stream_in, queries, new_keys, new_values, key_cache, value_cache, lengths, out_weight, norm_gain
):
    batch, steps, width = queries.shape
    block_len, kv, hd = key_cache.shape[1:]
    heads = width // hd
    depth, cw = out_weight.shape
    own_w = stream_in.shape[2]
    rows = batch * steps
    k_own = n_rep // n_tp
    assert n_rep & (n_rep - 1) == 0
    assert n_rep % n_tp == 0 and k_own % 2 == 0 and n_tp % 2 == 0 and heads % n_tp == 0
    assert batch <= TILE and k_own <= TILE and rows <= LANES and n_tp * TILE <= LANES
    owned = heads // n_tp
    orow = owned * steps
    hs = heads * steps
    cached = block_len * kv
    assert cached % LANES == 0 and LANES % kv == 0 and steps * kv <= PAD and hs % LANES == 0
    q = queries.reshape(batch, steps, heads, hd).transpose(0, 2, 1, 3).reshape(batch, hs, hd)
    nk = new_keys.reshape(batch, steps * kv, hd)
    nv = new_values.reshape(batch, steps * kv, hd)
    kc = key_cache.reshape(batch, cached, hd)
    vc = value_cache.reshape(batch, cached, hd)
    cfg = (n_rep, n_tp, batch, steps, heads, kv, block_len, own_w * n_tp, 1e-6)
    pairs = n_rep // 2
    order = [[0], [1], [2, 3]] if pairs == 4 else [[p] for p in range(pairs)]
    far = [m for p in range(pairs - 1, -1, -1) for m in (2 * p + 1, 2 * p) if m]
    bf, f32 = jnp.bfloat16, jnp.float32
    anyspec = pl.BlockSpec(memory_space=pl.ANY)
    vmem = pl.BlockSpec(memory_space=pltpu.VMEM)
    hidden, scale = pl.pallas_call(
        functools.partial(kernel, cfg, order, far),
        out_shape=(
            pltpu.VMEM(stream_in.shape, f32),
            pltpu.VMEM(stream_in.shape, f32),
        ),
        in_specs=[anyspec] * 9,
        out_specs=(vmem, vmem),
        scratch_shapes=[
            pltpu.SMEM((batch,), jnp.int32),
            pltpu.VMEM((batch, hs, hd), bf),
            pltpu.VMEM((batch, 2, cached + PAD, hd), bf),
            pltpu.VMEM((depth, cw), bf),
            pltpu.VMEM((own_w // 128, 128), bf),
            pltpu.VMEM((n_tp, batch, orow, hd), bf),
            pltpu.VMEM((n_tp - 1, batch, orow, hd), bf),
            pltpu.VMEM((TILE, hs), f32),
            pltpu.VMEM((n_tp - 1, TILE, hs), f32),
            pltpu.VMEM((hs, LANES), f32),
            pltpu.VMEM((n_rep, rows, depth), bf),
            pltpu.VMEM((pairs, 2, rows, cw), bf),
            pltpu.VMEM((pairs, rows, cw), bf),
            pltpu.VMEM((pairs, rows, cw), bf),
            pltpu.VMEM((n_rep // 2, rows, cw), bf),
            pltpu.VMEM((batch, steps, own_w), bf),
            pltpu.VMEM((1, LANES), f32),
            pltpu.VMEM((n_tp, LANES), f32),
            pltpu.SemaphoreType.DMA((LOADS + batch + SINGLES + 2 * pairs,)),
        ],
        compiler_params=pltpu.CompilerParams(collective_id=0, has_side_effects=True),
    )(lengths, q, nk, nv, kc, vc, out_weight, stream_in, norm_gain.reshape(own_w // 128, 128))
    return (hidden.astype(bf), (hidden * scale).astype(bf))


def solution(mesh):
    return jax.shard_map(
        functools.partial(on_device, mesh.shape["rep"], mesh.shape["tp"]),
        mesh=mesh,
        in_specs=(
            P("rep", None, "tp"),
            P("rep", None, None),
            P("rep", None, None, None),
            P("rep", None, None, None),
            P("rep", "tp", None, None),
            P("rep", "tp", None, None),
            P("rep"),
            P("tp", "rep"),
            P("tp"),
        ),
        out_specs=(P("rep", None, "tp"), P("rep", None, "tp")),
        check_vma=False,
    )
```

```python
import functools
import math

import jax
import jax.numpy as jnp
from jax import lax
from jax.experimental import pallas as pl
from jax.experimental.pallas import tpu as pltpu
from jax.sharding import PartitionSpec as P

MESH = pl.DeviceIdType.MESH
PAD = 128
LANES = 128
LEAD = 1
TILE = 8
LOADS = 5
SINGLES = 10


def flip(index, mask, count):
    other = 0
    bit = 1
    while bit < count:
        digit = (index // bit) % 2
        other = other + bit * ((1 - digit) if mask & bit else digit)
        bit *= 2
    return other


def landed(ref, sem):
    pltpu.make_async_copy(ref, ref, sem).wait()


def attend(cfg, b, length, tp, q_v, kv_v):
    n_rep, n_tp, batch, steps, heads, kv, block_len, width_all, eps = cfg
    hd = q_v.shape[2]
    group = steps * (heads // kv)
    cached = block_len * kv
    fresh = steps * kv
    chunks = cached // LANES
    scaling = 1.0 / math.sqrt(hd)
    lane = lax.broadcasted_iota(jnp.int32, (group, LANES), 1)
    row = lax.broadcasted_iota(jnp.int32, (group, LANES), 0)
    kind = lane % kv
    place = lane // kv
    causal = (place <= row % steps) & (lane < fresh) & (tp == 0)
    s = lax.dot_general(
        q_v[b], kv_v[b, 0], (((1,), (1,)), ((), ())), preferred_element_type=jnp.float32
    )
    left = length - tp * block_len
    kept = []
    for c in range(chunks + 1):
        own = s[0:group, c * LANES : (c + 1) * LANES]
        for g in range(1, kv):
            own = jnp.where(kind == g, s[g * group : (g + 1) * group, c * LANES : (c + 1) * LANES], own)
        seen = place < left - c * (LANES // kv) if c < chunks else causal
        kept.append(jnp.where(seen, own, -1e30))
    highest = functools.reduce(jnp.maximum, kept)
    tops = [jnp.max(jnp.where(kind == g, highest, -3e38), axis=1, keepdims=True) for g in range(kv)]
    top = jnp.broadcast_to(tops[0], (group, LANES))
    for g in range(1, kv):
        top = jnp.where(kind == g, tops[g], top)
    weights = [jnp.exp((k - top) * scaling) for k in kept]
    summed = functools.reduce(jnp.add, weights)
    totals = [jnp.sum(jnp.where(kind == g, summed, 0.0), axis=1, keepdims=True) for g in range(kv)]
    rounded = jnp.concatenate([w.astype(jnp.bfloat16) for w in weights], axis=1)
    one = jnp.where(kind == 0, 1.0, 0.0)
    spread = []
    for g in range(kv):
        one = jnp.where(kind == g, 1.0, 0.0).astype(jnp.bfloat16)
        spread.append(rounded * jnp.concatenate([one] * (chunks + 1), axis=1))
    spread = jnp.concatenate(spread, axis=0)
    num = jnp.dot(spread, kv_v[b, 1], preferred_element_type=jnp.float32)
    total = jnp.concatenate(totals, axis=0)
    return (num / total).astype(jnp.bfloat16), jnp.concatenate(tops, axis=0) * scaling + jnp.log(total)


def kernel(
    cfg, order, far,
    len_hbm, q_hbm, nk_hbm, nv_hbm, k_hbm, v_hbm, w_hbm, x_hbm, gain_hbm,
    hidden_ref, scale_ref,
    len_s, q_v, kv_v, w_v, gain_v,
    send_o, recv_o, send_l, recv_l, mix,
    gathered, parts, other, ready, recv_c, x_v, sq_s, sq_r,
    sems, news,
):
    n_rep, n_tp, batch, steps, heads, kv, block_len, width_all, eps = cfg
    rep = lax.axis_index("rep")
    tp = lax.axis_index("tp")
    k_own = n_rep // n_tp
    pairs = n_rep // 2
    rows = batch * steps
    owned = heads // n_tp
    orow = owned * steps
    hs = heads * steps
    cached = block_len * kv
    fresh = steps * kv
    cw = w_v.shape[1]
    hd = q_v.shape[2]
    owner = rep // k_own
    core = lax.rem(tp, 2)
    chips = n_tp // 2
    line = rep // 2
    half = pairs // 2
    is_own = (owner == tp) & (core == 0)
    not_own = jnp.logical_not(is_own)
    slot = lax.rem(rep, k_own) * chips + tp // 2

    s_len, s_q, s_w, s_gain, s_x = (sems.at[i] for i in range(LOADS))
    s_kv = [sems.at[LOADS + b] for b in range(batch)]
    first = LOADS + batch
    (ao_s, ao_r, al_s, al_r, b_s, d_s, c_s, c_r, q_s, q_r) = (
        sems.at[first + i] for i in range(SINGLES)
    )
    first += SINGLES
    b_r = [sems.at[first + p] for p in range(pairs)]
    d_r = [sems.at[first + pairs + p] for p in range(pairs)]

    loads = [pltpu.make_async_copy(q_hbm, q_v, s_q)]
    for b in range(batch):
        loads += [
            pltpu.make_async_copy(k_hbm.at[b], kv_v.at[b, 0, pl.ds(0, cached)], s_kv[b]),
            pltpu.make_async_copy(nk_hbm.at[b], kv_v.at[b, 0, pl.ds(cached, fresh)], s_kv[b]),
            pltpu.make_async_copy(v_hbm.at[b], kv_v.at[b, 1, pl.ds(0, cached)], s_kv[b]),
            pltpu.make_async_copy(nv_hbm.at[b], kv_v.at[b, 1, pl.ds(cached, fresh)], s_kv[b]),
        ]
        if b == 0:
            loads.append(pltpu.make_async_copy(len_hbm, len_s, s_len))
    loads += [
        pltpu.make_async_copy(w_hbm, w_v, s_w),
        pltpu.make_async_copy(gain_hbm, gain_v, s_gain),
        pltpu.make_async_copy(x_hbm, x_v, s_x),
    ]
    for c in loads:
        c.start()

    barrier = pltpu.get_barrier_semaphore()
    leads = tp == LEAD

    def greet(group):
        pl.semaphore_signal(barrier, inc=1, device_id=(group, LEAD), device_id_type=MESH)

    for j in range(n_rep - 1, 0, -1):
        greet(lax.rem(rep + j, n_rep))

    @pl.when(jnp.logical_not(leads))
    def _():
        greet(rep)

    for j in range(1, n_tp):
        peer = lax.rem(tp + j, n_tp)

        @pl.when(peer != LEAD)
        def _():
            pl.semaphore_signal(barrier, inc=1, device_id=(rep, peer), device_id_type=MESH)

    for b in range(batch):
        for i in range(2):
            kv_v[b, i, cached + fresh : cached + PAD, :] = jnp.zeros((PAD - fresh, hd), jnp.bfloat16)

    lane = lax.broadcasted_iota(jnp.int32, (hs, LANES), 1)
    lse = jnp.zeros((hs, LANES), jnp.float32)
    landed(len_s, s_len)
    landed(q_v, s_q)
    together = 1
    for b0 in range(0, batch, together):
        for b in range(b0, b0 + together):
            landed(kv_v.at[b, :, pl.ds(0, cached + fresh)], s_kv[b])
        for b in range(b0, b0 + together):
            out, value = attend(cfg, b, len_s[b], tp, q_v, kv_v)
            for t in range(n_tp):
                send_o[t, b] = out[t * orow : (t + 1) * orow]
            lse = jnp.where(lane == b, value, lse)
        if b0 == 0:
            @pl.when(jnp.logical_not(leads))
            def _():
                pl.semaphore_wait(barrier, n_tp - 1)
                pl.semaphore_signal(news, inc=1, device_id=(rep, LEAD), device_id_type=MESH)
    send_l[...] = lse.T[:TILE]

    @pl.when(leads)
    def _():
        pl.semaphore_wait(news, n_tp - 1)

    for j in range(1, n_tp):
        peer = lax.rem(tp + j, n_tp)
        pltpu.make_async_remote_copy(
            send_l, recv_l.at[j - 1], al_s, al_r, device_id=(rep, peer), device_id_type=MESH).start()
        pltpu.make_async_remote_copy(
            send_o.at[peer], recv_o.at[j - 1], ao_s, ao_r, device_id=(rep, peer), device_id_type=MESH).start()

    @pl.when(leads)
    def _():
        pl.semaphore_wait(barrier, n_rep * n_tp - 1)
        for j in range(1, n_tp):
            pl.semaphore_signal(news, inc=1, device_id=(rep, lax.rem(tp + j, n_tp)), device_id_type=MESH)

    landed(recv_l, al_r)
    ls = [send_l[...]] + [recv_l[j] for j in range(n_tp - 1)]
    most = functools.reduce(jnp.maximum, ls)
    ws = [jnp.exp(l - most) for l in ls]
    inv = 1.0 / functools.reduce(jnp.add, ws)
    ws = [w * inv for w in ws]
    if n_tp * TILE < LANES:
        ws.append(jnp.zeros((LANES - n_tp * TILE, hs), jnp.float32))
    mix[...] = jnp.concatenate(ws, axis=0).T
    share = mix[pl.ds(pl.multiple_of(tp * orow, orow), orow), :]
    landed(recv_o, ao_r)
    att = []
    for b in range(batch):
        acc = share[:, b : b + 1] * send_o[tp, b].astype(jnp.float32)
        for j in range(1, n_tp):
            acc = acc + share[:, j * TILE + b : j * TILE + b + 1] * recv_o[j - 1, b].astype(jnp.float32)
        att.append(acc.astype(jnp.bfloat16))
    att = jnp.concatenate(att, axis=0)
    m = batch * orow
    to = lax.broadcasted_iota(jnp.int32, (m, m), 0)
    frm = lax.broadcasted_iota(jnp.int32, (m, m), 1)
    want = ((to // steps) % batch) * orow + (to // rows) * steps + to % steps
    pick = jnp.where(frm == want, 1.0, 0.0).astype(jnp.bfloat16)
    att = jnp.dot(pick, att, preferred_element_type=jnp.float32).astype(jnp.bfloat16)
    gathered[rep] = jnp.concatenate([att[h * rows : (h + 1) * rows] for h in range(owned)], axis=1)

    @pl.when(jnp.logical_not(leads))
    def _():
        pl.semaphore_wait(news, 1)

    for mask in far:
        pltpu.make_async_remote_copy(
            gathered.at[rep], gathered.at[rep], b_s, sems.at[first + rep // 2],
            device_id=(flip(rep, mask, n_rep), tp), device_id_type=MESH).start()
    partner = tp + 1 - 2 * core

    def keeper(p):
        return ((line < half) if p >= half else (line >= half)).astype(jnp.int32)

    def pass_on(p, when):
        @pl.when(when & (core == keeper(p)))
        def _():
            landed(other.at[p], d_r[p])
            for i in range(2):
                both = parts[p, i].astype(jnp.float32) + other[p, i].astype(jnp.float32)
                ready[p, i] = both.astype(jnp.bfloat16)
                local = is_own & (rep == 2 * p + i)

                @pl.when(jnp.logical_not(local))
                def _():
                    pltpu.make_async_remote_copy(
                        ready.at[p, i], recv_c.at[slot], c_s, c_r,
                        device_id=(2 * p + i, owner), device_id_type=MESH).start()

                @pl.when(local)
                def _():
                    recv_c[slot] = ready[p, i]

    landed(w_v, s_w)
    waiting = []
    for batch_of in order:
        distant = functools.reduce(jnp.logical_or, [jnp.abs(line - p) > 1 for p in batch_of])
        for p in waiting:
            pass_on(p, distant)
        for p in batch_of:
            mine = rep // 2 == p

            @pl.when(mine)
            def _():
                landed(gathered.at[0], b_r[p])

            @pl.when(jnp.logical_not(mine))
            def _():
                landed(gathered.at[pl.ds(2 * p, 2)], b_r[p])

        block = jnp.concatenate([gathered[2 * p + i] for p in batch_of for i in range(2)], axis=0)
        proj = jnp.dot(block, w_v[...], preferred_element_type=jnp.float32).astype(jnp.bfloat16)
        for n, p in enumerate(batch_of):
            for i in range(2):
                parts[p, i] = proj[(2 * n + i) * rows : (2 * n + i + 1) * rows]
            @pl.when(core != keeper(p))
            def _():
                pltpu.make_async_remote_copy(
                    parts.at[p], other.at[p], d_s, d_r[p],
                    device_id=(rep, partner), device_id_type=MESH).start()

        for p in waiting:
            pass_on(p, jnp.logical_not(distant))
        waiting = batch_of
    for p in waiting:
        pass_on(p, line >= 0)

    landed(x_v, s_x)
    landed(gain_v, s_gain)
    gain = gain_v[...].astype(jnp.float32)
    gain = jnp.concatenate([gain[c : c + 1] for c in range(gain.shape[0])], axis=1)

    x = x_v[...].astype(jnp.float32).reshape(rows, x_v.shape[2])
    spot = lax.broadcasted_iota(jnp.int32, (rows, LANES), 0) == lax.broadcasted_iota(jnp.int32, (rows, LANES), 1)

    @pl.when(is_own)
    def _():
        landed(recv_c.at[pl.ds(0, n_rep // 2 - 1)], c_r)

    @pl.when(not_own)
    def _():
        landed(recv_c, c_r)

    pieces = []
    for i in range(k_own):
        acc = recv_c[i * chips].astype(jnp.float32)
        for h in range(1, chips):
            acc = acc + recv_c[i * chips + h].astype(jnp.float32)
        pieces.append(acc)
    hidden = x + jnp.concatenate(pieces, axis=1)
    squares = jnp.sum(hidden * hidden, axis=1, keepdims=True)
    sq_s[...] = jnp.sum(jnp.where(spot, squares, 0.0), axis=0, keepdims=True)
    for j in range(1, n_tp):
        pltpu.make_async_remote_copy(
            sq_s, sq_r.at[pl.ds(j, 1)], q_s, q_r,
            device_id=(rep, lax.rem(tp + j, n_tp)), device_id_type=MESH).start()
    sq_r[0:1, :] = sq_s[...]
    hidden_ref[...] = hidden.reshape(hidden_ref.shape)
    landed(sq_r.at[pl.ds(1, n_tp - 1)], q_r)
    every = jnp.sum(sq_r[...], axis=0, keepdims=True)
    every = jnp.sum(jnp.where(spot, every, 0.0), axis=1, keepdims=True)
    inverse = lax.rsqrt(every / width_all + eps)
    scale_ref[...] = (inverse * gain).reshape(scale_ref.shape)

    landed(recv_l, al_s)
    landed(recv_o, ao_s)
    landed(gathered.at[pl.ds(1, n_rep - 1)], b_s)
    landed(other.at[pl.ds(0, half)], d_s)
    landed(sq_r.at[pl.ds(1, n_tp - 1)], q_s)

    @pl.when(is_own)
    def _():
        landed(recv_c.at[pl.ds(0, n_rep // 2 - 1)], c_s)

    @pl.when(not_own)
    def _():
        landed(recv_c, c_s)


def on_device(
    n_rep, n_tp,
    stream_in, queries, new_keys, new_values, key_cache, value_cache, lengths, out_weight, norm_gain
):
    batch, steps, width = queries.shape
    block_len, kv, hd = key_cache.shape[1:]
    heads = width // hd
    depth, cw = out_weight.shape
    own_w = stream_in.shape[2]
    rows = batch * steps
    k_own = n_rep // n_tp
    assert n_rep & (n_rep - 1) == 0
    assert n_rep % n_tp == 0 and k_own % 2 == 0 and n_tp % 2 == 0 and heads % n_tp == 0
    assert batch <= TILE and k_own <= TILE and rows <= LANES and n_tp * TILE <= LANES
    owned = heads // n_tp
    orow = owned * steps
    hs = heads * steps
    cached = block_len * kv
    assert cached % LANES == 0 and LANES % kv == 0 and steps * kv <= PAD and hs % LANES == 0
    q = queries.reshape(batch, steps, heads, hd).transpose(0, 2, 1, 3).reshape(batch, hs, hd)
    nk = new_keys.reshape(batch, steps * kv, hd)
    nv = new_values.reshape(batch, steps * kv, hd)
    kc = key_cache.reshape(batch, cached, hd)
    vc = value_cache.reshape(batch, cached, hd)
    cfg = (n_rep, n_tp, batch, steps, heads, kv, block_len, own_w * n_tp, 1e-6)
    pairs = n_rep // 2
    order = [[0], [1], [2, 3]] if pairs == 4 else [[p] for p in range(pairs)]
    far = [m for p in range(pairs - 1, -1, -1) for m in (2 * p + 1, 2 * p) if m]
    bf, f32 = jnp.bfloat16, jnp.float32
    anyspec = pl.BlockSpec(memory_space=pl.ANY)
    vmem = pl.BlockSpec(memory_space=pltpu.VMEM)
    hidden, scale = pl.pallas_call(
        functools.partial(kernel, cfg, order, far),
        out_shape=(
            pltpu.VMEM(stream_in.shape, f32),
            pltpu.VMEM(stream_in.shape, f32),
        ),
        in_specs=[anyspec] * 9,
        out_specs=(vmem, vmem),
        scratch_shapes=[
            pltpu.SMEM((batch,), jnp.int32),
            pltpu.VMEM((batch, hs, hd), bf),
            pltpu.VMEM((batch, 2, cached + PAD, hd), bf),
            pltpu.VMEM((depth, cw), bf),
            pltpu.VMEM((own_w // 128, 128), bf),
            pltpu.VMEM((n_tp, batch, orow, hd), bf),
            pltpu.VMEM((n_tp - 1, batch, orow, hd), bf),
            pltpu.VMEM((TILE, hs), f32),
            pltpu.VMEM((n_tp - 1, TILE, hs), f32),
            pltpu.VMEM((hs, LANES), f32),
            pltpu.VMEM((n_rep, rows, depth), bf),
            pltpu.VMEM((pairs, 2, rows, cw), bf),
            pltpu.VMEM((pairs, 2, rows, cw), bf),
            pltpu.VMEM((pairs, 2, rows, cw), bf),
            pltpu.VMEM((n_rep // 2, rows, cw), bf),
            pltpu.VMEM((batch, steps, own_w), bf),
            pltpu.VMEM((1, LANES), f32),
            pltpu.VMEM((n_tp, LANES), f32),
            pltpu.SemaphoreType.DMA((LOADS + batch + SINGLES + 2 * pairs,)),
            pltpu.SemaphoreType.REGULAR,
        ],
        compiler_params=pltpu.CompilerParams(collective_id=0, has_side_effects=True),
    )(lengths, q, nk, nv, kc, vc, out_weight, stream_in, norm_gain.reshape(own_w // 128, 128))
    return (hidden.astype(bf), (hidden * scale).astype(bf))


def solution(mesh):
    return jax.shard_map(
        functools.partial(on_device, mesh.shape["rep"], mesh.shape["tp"]),
        mesh=mesh,
        in_specs=(
            P("rep", None, "tp"),
            P("rep", None, None),
            P("rep", None, None, None),
            P("rep", None, None, None),
            P("rep", "tp", None, None),
            P("rep", "tp", None, None),
            P("rep"),
            P("tp", "rep"),
            P("tp"),
        ),
        out_specs=(P("rep", None, "tp"), P("rep", None, "tp")),
        check_vma=False,
    )
```

```python
import functools
import math

import jax
import jax.numpy as jnp
from jax import lax
from jax.experimental import pallas as pl
from jax.experimental.pallas import tpu as pltpu
from jax.sharding import PartitionSpec as P

MESH = pl.DeviceIdType.MESH
PAD = 128
LANES = 128
LEAD = 1
TILE = 8
LOADS = 5
SINGLES = 10


def flip(index, mask, count):
    other = 0
    bit = 1
    while bit < count:
        digit = (index // bit) % 2
        other = other + bit * ((1 - digit) if mask & bit else digit)
        bit *= 2
    return other


def landed(ref, sem):
    pltpu.make_async_copy(ref, ref, sem).wait()


def lanes_of(cfg):
    n_rep, n_tp, batch, steps, heads, kv, block_len, width_all, eps = cfg
    group = steps * (heads // kv)
    lane = lax.broadcasted_iota(jnp.int32, (group, LANES), 1)
    row = lax.broadcasted_iota(jnp.int32, (group, LANES), 0)
    return group, lane, row, lane % kv, lane // kv


def score(cfg, b, length, tp, q_v, kv_v):
    n_rep, n_tp, batch, steps, heads, kv, block_len, width_all, eps = cfg
    group, lane, row, kind, place = lanes_of(cfg)
    chunks = block_len * kv // LANES
    causal = (place <= row % steps) & (lane < steps * kv) & (tp == 0)
    s = lax.dot_general(
        q_v[b], kv_v[b, 0], (((1,), (1,)), ((), ())), preferred_element_type=jnp.float32
    )
    left = length - tp * block_len
    kept = []
    for c in range(chunks + 1):
        own = s[0:group, c * LANES : (c + 1) * LANES]
        for g in range(1, kv):
            own = jnp.where(kind == g, s[g * group : (g + 1) * group, c * LANES : (c + 1) * LANES], own)
        seen = place < left - c * (LANES // kv) if c < chunks else causal
        kept.append(jnp.where(seen, own, -1e30))
    return kept


def soften(cfg, kept, scaling):
    kv = cfg[5]
    group, lane, row, kind, place = lanes_of(cfg)
    highest = functools.reduce(jnp.maximum, kept)
    tops = [jnp.max(jnp.where(kind == g, highest, -3e38), axis=1, keepdims=True) for g in range(kv)]
    top = jnp.broadcast_to(tops[0], (group, LANES))
    for g in range(1, kv):
        top = jnp.where(kind == g, tops[g], top)
    weights = [jnp.exp((k - top) * scaling) for k in kept]
    summed = functools.reduce(jnp.add, weights)
    totals = [jnp.sum(jnp.where(kind == g, summed, 0.0), axis=1, keepdims=True) for g in range(kv)]
    rounded = [w.astype(jnp.bfloat16) for w in weights]
    return rounded, jnp.concatenate(tops, axis=0), jnp.concatenate(totals, axis=0)


def blend(cfg, rounded, values):
    kv = cfg[5]
    group, lane, row, kind, place = lanes_of(cfg)
    spread = []
    for g in range(kv):
        one = jnp.where(kind == g, 1.0, 0.0).astype(jnp.bfloat16)
        spread.append(jnp.concatenate([w * one for w in rounded], axis=1))
    spread = jnp.concatenate(spread, axis=0)
    return jnp.dot(spread, values, preferred_element_type=jnp.float32)


def kernel(
    cfg, order, far,
    len_hbm, q_hbm, nk_hbm, nv_hbm, k_hbm, v_hbm, w_hbm, x_hbm, gain_hbm,
    hidden_ref, scale_ref,
    len_s, q_v, kv_v, w_v, gain_v,
    send_o, recv_o, send_l, recv_l, mix,
    gathered, parts, other, ready, recv_c, x_v, sq_s, sq_r,
    sems, news,
):
    n_rep, n_tp, batch, steps, heads, kv, block_len, width_all, eps = cfg
    rep = lax.axis_index("rep")
    tp = lax.axis_index("tp")
    k_own = n_rep // n_tp
    pairs = n_rep // 2
    rows = batch * steps
    owned = heads // n_tp
    orow = owned * steps
    hs = heads * steps
    cached = block_len * kv
    fresh = steps * kv
    cw = w_v.shape[1]
    hd = q_v.shape[2]
    owner = rep // k_own
    core = lax.rem(tp, 2)
    chips = n_tp // 2
    line = rep // 2
    half = pairs // 2
    is_own = (owner == tp) & (core == 0)
    not_own = jnp.logical_not(is_own)
    slot = lax.rem(rep, k_own) * chips + tp // 2

    s_len, s_q, s_w, s_gain, s_x = (sems.at[i] for i in range(LOADS))
    s_kv = [sems.at[LOADS + b] for b in range(batch)]
    s_vv = [sems.at[LOADS + batch + b] for b in range(batch)]
    first = LOADS + 2 * batch
    (ao_s, ao_r, al_s, al_r, b_s, d_s, c_s, c_r, q_s, q_r) = (
        sems.at[first + i] for i in range(SINGLES)
    )
    first += SINGLES
    b_r = [sems.at[first + p] for p in range(pairs)]
    d_r = [sems.at[first + pairs + p] for p in range(pairs)]
    z_r = [sems.at[first + 2 * pairs + p] for p in range(pairs)]

    loads = [pltpu.make_async_copy(q_hbm, q_v, s_q)]
    for b0 in range(0, batch, batch):
        for i, old, new, marks in ((0, k_hbm, nk_hbm, s_kv), (1, v_hbm, nv_hbm, s_vv)):
            for b in range(b0, b0 + batch):
                loads += [
                    pltpu.make_async_copy(old.at[b], kv_v.at[b, i, pl.ds(0, cached)], marks[b]),
                    pltpu.make_async_copy(new.at[b], kv_v.at[b, i, pl.ds(cached, fresh)], marks[b]),
                ]
        if b0 == 0:
            loads.append(pltpu.make_async_copy(len_hbm, len_s, s_len))
    loads += [
        pltpu.make_async_copy(w_hbm, w_v, s_w),
        pltpu.make_async_copy(gain_hbm, gain_v, s_gain),
        pltpu.make_async_copy(x_hbm, x_v, s_x),
    ]
    for c in loads:
        c.start()

    barrier = pltpu.get_barrier_semaphore()
    leads = tp == LEAD

    def greet(group):
        pl.semaphore_signal(barrier, inc=1, device_id=(group, LEAD), device_id_type=MESH)

    for j in range(n_rep - 1, 0, -1):
        greet(lax.rem(rep + j, n_rep))

    @pl.when(jnp.logical_not(leads))
    def _():
        greet(rep)

    for j in range(1, n_tp):
        peer = lax.rem(tp + j, n_tp)

        @pl.when(peer != LEAD)
        def _():
            pl.semaphore_signal(barrier, inc=1, device_id=(rep, peer), device_id_type=MESH)

    for b in range(batch):
        for i in range(2):
            kv_v[b, i, cached + fresh : cached + PAD, :] = jnp.zeros((PAD - fresh, hd), jnp.bfloat16)

    lane = lax.broadcasted_iota(jnp.int32, (hs, LANES), 1)
    lse = jnp.zeros((hs, LANES), jnp.float32)
    landed(len_s, s_len)
    landed(q_v, s_q)
    scaling = 1.0 / math.sqrt(hd)
    together = batch
    for b0 in range(0, batch, together):
        span = range(b0, b0 + together)
        kept = []
        for b in span:
            landed(kv_v.at[b, 0, pl.ds(0, cached + fresh)], s_kv[b])
            kept.append(score(cfg, b, len_s[b], tp, q_v, kv_v))
        soft = [soften(cfg, k, scaling) for k in kept]
        for b in span:
            landed(kv_v.at[b, 1, pl.ds(0, cached + fresh)], s_vv[b])
        if b0 == 0:
            @pl.when(jnp.logical_not(leads))
            def _():
                pl.semaphore_wait(barrier, n_tp - 1)
                pl.semaphore_signal(news, inc=1, device_id=(rep, LEAD), device_id_type=MESH)
        nums = [blend(cfg, soft[i][0], kv_v[b, 1]) for i, b in enumerate(span)]
        for i, b in enumerate(span):
            rounded, tops, total = soft[i]
            out = (nums[i] / total).astype(jnp.bfloat16)
            for t in range(n_tp):
                send_o[t, b] = out[t * orow : (t + 1) * orow]
            lse = jnp.where(lane == b, tops * scaling + jnp.log(total), lse)
    send_l[...] = lse.T[:TILE]

    @pl.when(leads)
    def _():
        pl.semaphore_wait(news, n_tp - 1)

    for j in range(1, n_tp):
        peer = lax.rem(tp + j, n_tp)
        pltpu.make_async_remote_copy(
            send_l, recv_l.at[j - 1], al_s, al_r, device_id=(rep, peer), device_id_type=MESH).start()
        pltpu.make_async_remote_copy(
            send_o.at[peer], recv_o.at[j - 1], ao_s, ao_r, device_id=(rep, peer), device_id_type=MESH).start()

    @pl.when(leads)
    def _():
        pl.semaphore_wait(barrier, n_rep * n_tp - 1)
        for j in range(1, n_tp):
            pl.semaphore_signal(news, inc=1, device_id=(rep, lax.rem(tp + j, n_tp)), device_id_type=MESH)

    landed(recv_l, al_r)
    ls = [send_l[...]] + [recv_l[j] for j in range(n_tp - 1)]
    most = functools.reduce(jnp.maximum, ls)
    ws = [jnp.exp(l - most) for l in ls]
    inv = 1.0 / functools.reduce(jnp.add, ws)
    ws = [w * inv for w in ws]
    if n_tp * TILE < LANES:
        ws.append(jnp.zeros((LANES - n_tp * TILE, hs), jnp.float32))
    mix[...] = jnp.concatenate(ws, axis=0).T
    share = mix[pl.ds(pl.multiple_of(tp * orow, orow), orow), :]
    landed(recv_o, ao_r)
    att = []
    for b in range(batch):
        acc = share[:, b : b + 1] * send_o[tp, b].astype(jnp.float32)
        for j in range(1, n_tp):
            acc = acc + share[:, j * TILE + b : j * TILE + b + 1] * recv_o[j - 1, b].astype(jnp.float32)
        att.append(acc.astype(jnp.bfloat16))
    att = jnp.concatenate(att, axis=0)
    m = batch * orow
    to = lax.broadcasted_iota(jnp.int32, (m, m), 0)
    frm = lax.broadcasted_iota(jnp.int32, (m, m), 1)
    want = ((to // steps) % batch) * orow + (to // rows) * steps + to % steps
    pick = jnp.where(frm == want, 1.0, 0.0).astype(jnp.bfloat16)
    att = jnp.dot(pick, att, preferred_element_type=jnp.float32).astype(jnp.bfloat16)
    gathered[rep] = jnp.concatenate([att[h * rows : (h + 1) * rows] for h in range(owned)], axis=1)

    @pl.when(jnp.logical_not(leads))
    def _():
        pl.semaphore_wait(news, 1)

    side = lax.rem(rep, 2)
    across = 2 * line + 1 - side
    relays = core == 1

    def share(source, target, sem):
        pltpu.make_async_remote_copy(
            gathered.at[source], gathered.at[source], b_s, sem,
            device_id=(target, tp), device_id_type=MESH).start()

    def relay(p):
        landed(gathered.at[p], z_r[p])
        share(2 * p + side, across, b_r[p])

    for mask in far:
        there = flip(line, mask, pairs)
        share(rep, 2 * there + side, sems.at[first + 2 * pairs + line])
        if mask < half:
            share(rep, 2 * there + 1 - side, sems.at[first + line])
        else:
            @pl.when(jnp.logical_not(relays & (line >= half)))
            def _():
                share(rep, 2 * there + 1 - side, sems.at[first + line])

    share(rep, across, sems.at[first + line])

    partner = tp + 1 - 2 * core

    def keeper(p):
        return ((line < half) if p >= half else (line >= half)).astype(jnp.int32)

    def pass_on(p, when):
        @pl.when(when & (core == keeper(p)))
        def _():
            landed(other.at[p], d_r[p])
            for i in range(2):
                both = parts[p, i].astype(jnp.float32) + other[p, i].astype(jnp.float32)
                ready[p, i] = both.astype(jnp.bfloat16)
                local = is_own & (rep == 2 * p + i)

                @pl.when(jnp.logical_not(local))
                def _():
                    pltpu.make_async_remote_copy(
                        ready.at[p, i], recv_c.at[slot], c_s, c_r,
                        device_id=(2 * p + i, owner), device_id_type=MESH).start()

                @pl.when(local)
                def _():
                    recv_c[slot] = ready[p, i]

    landed(w_v, s_w)
    waiting = []
    for batch_of in order:
        distant = functools.reduce(jnp.logical_or, [jnp.abs(line - p) > 1 for p in batch_of])
        for p in waiting:
            pass_on(p, distant)
        for p in batch_of:
            if p == pairs - 1:
                @pl.when(relays & (line < half))
                def _():
                    for q in range(pairs - 1, half - 1, -1):
                        relay(q)

            passed = line == p
            if p >= half:
                passed = passed | (relays & (line < half))

            @pl.when(jnp.logical_not(passed))
            def _():
                landed(gathered.at[2 * p], z_r[p])

            landed(gathered.at[2 * p], b_r[p])

        block = jnp.concatenate([gathered[2 * p + i] for p in batch_of for i in range(2)], axis=0)
        proj = jnp.dot(block, w_v[...], preferred_element_type=jnp.float32).astype(jnp.bfloat16)
        for n, p in enumerate(batch_of):
            for i in range(2):
                parts[p, i] = proj[(2 * n + i) * rows : (2 * n + i + 1) * rows]
            @pl.when(core != keeper(p))
            def _():
                pltpu.make_async_remote_copy(
                    parts.at[p], other.at[p], d_s, d_r[p],
                    device_id=(rep, partner), device_id_type=MESH).start()

        for p in waiting:
            pass_on(p, jnp.logical_not(distant))
        waiting = batch_of
    for p in waiting:
        pass_on(p, line >= 0)

    landed(x_v, s_x)
    landed(gain_v, s_gain)
    gain = gain_v[...].astype(jnp.float32)
    gain = jnp.concatenate([gain[c : c + 1] for c in range(gain.shape[0])], axis=1)

    x = x_v[...].astype(jnp.float32).reshape(rows, x_v.shape[2])
    spot = lax.broadcasted_iota(jnp.int32, (rows, LANES), 0) == lax.broadcasted_iota(jnp.int32, (rows, LANES), 1)

    @pl.when(is_own)
    def _():
        landed(recv_c.at[pl.ds(0, n_rep // 2 - 1)], c_r)

    @pl.when(not_own)
    def _():
        landed(recv_c, c_r)

    pieces = []
    for i in range(k_own):
        acc = recv_c[i * chips].astype(jnp.float32)
        for h in range(1, chips):
            acc = acc + recv_c[i * chips + h].astype(jnp.float32)
        pieces.append(acc)
    hidden = x + jnp.concatenate(pieces, axis=1)
    squares = jnp.sum(hidden * hidden, axis=1, keepdims=True)
    sq_s[...] = jnp.sum(jnp.where(spot, squares, 0.0), axis=0, keepdims=True)
    for j in range(1, n_tp):
        pltpu.make_async_remote_copy(
            sq_s, sq_r.at[pl.ds(j, 1)], q_s, q_r,
            device_id=(rep, lax.rem(tp + j, n_tp)), device_id_type=MESH).start()
    sq_r[0:1, :] = sq_s[...]
    hidden_ref[...] = hidden.reshape(hidden_ref.shape)
    landed(sq_r.at[pl.ds(1, n_tp - 1)], q_r)
    every = jnp.sum(sq_r[...], axis=0, keepdims=True)
    every = jnp.sum(jnp.where(spot, every, 0.0), axis=1, keepdims=True)
    inverse = lax.rsqrt(every / width_all + eps)
    scale_ref[...] = (inverse * gain).reshape(scale_ref.shape)

    landed(recv_l, al_s)
    landed(recv_o, ao_s)
    landed(gathered.at[pl.ds(0, n_rep - 1 - half)], b_s)

    @pl.when(jnp.logical_not(relays & (line >= half)))
    def _():
        landed(gathered.at[pl.ds(0, half)], b_s)

    @pl.when(relays & (line < half))
    def _():
        landed(gathered.at[pl.ds(0, half)], b_s)

    landed(other.at[pl.ds(0, half)], d_s)
    landed(sq_r.at[pl.ds(1, n_tp - 1)], q_s)

    @pl.when(is_own)
    def _():
        landed(recv_c.at[pl.ds(0, n_rep // 2 - 1)], c_s)

    @pl.when(not_own)
    def _():
        landed(recv_c, c_s)


def on_device(
    n_rep, n_tp,
    stream_in, queries, new_keys, new_values, key_cache, value_cache, lengths, out_weight, norm_gain
):
    batch, steps, width = queries.shape
    block_len, kv, hd = key_cache.shape[1:]
    heads = width // hd
    depth, cw = out_weight.shape
    own_w = stream_in.shape[2]
    rows = batch * steps
    k_own = n_rep // n_tp
    assert n_rep & (n_rep - 1) == 0
    assert n_rep % n_tp == 0 and k_own % 2 == 0 and n_tp % 2 == 0 and heads % n_tp == 0
    assert batch <= TILE and k_own <= TILE and rows <= LANES and n_tp * TILE <= LANES
    owned = heads // n_tp
    orow = owned * steps
    hs = heads * steps
    cached = block_len * kv
    assert cached % LANES == 0 and LANES % kv == 0 and steps * kv <= PAD and hs % LANES == 0
    q = queries.reshape(batch, steps, heads, hd).transpose(0, 2, 1, 3).reshape(batch, hs, hd)
    nk = new_keys.reshape(batch, steps * kv, hd)
    nv = new_values.reshape(batch, steps * kv, hd)
    kc = key_cache.reshape(batch, cached, hd)
    vc = value_cache.reshape(batch, cached, hd)
    cfg = (n_rep, n_tp, batch, steps, heads, kv, block_len, own_w * n_tp, 1e-6)
    pairs = n_rep // 2
    half = pairs // 2
    order = [[0], [1], [3, 2]] if pairs == 4 else [[p] for p in [*range(half), *range(pairs - 1, half - 1, -1)]]
    far = [*range(pairs - 1, 0, -1)]
    bf, f32 = jnp.bfloat16, jnp.float32
    anyspec = pl.BlockSpec(memory_space=pl.ANY)
    vmem = pl.BlockSpec(memory_space=pltpu.VMEM)
    hidden, scale = pl.pallas_call(
        functools.partial(kernel, cfg, order, far),
        out_shape=(
            pltpu.VMEM(stream_in.shape, f32),
            pltpu.VMEM(stream_in.shape, f32),
        ),
        in_specs=[anyspec] * 9,
        out_specs=(vmem, vmem),
        scratch_shapes=[
            pltpu.SMEM((batch,), jnp.int32),
            pltpu.VMEM((batch, hs, hd), bf),
            pltpu.VMEM((batch, 2, cached + PAD, hd), bf),
            pltpu.VMEM((depth, cw), bf),
            pltpu.VMEM((own_w // 128, 128), bf),
            pltpu.VMEM((n_tp, batch, orow, hd), bf),
            pltpu.VMEM((n_tp - 1, batch, orow, hd), bf),
            pltpu.VMEM((TILE, hs), f32),
            pltpu.VMEM((n_tp - 1, TILE, hs), f32),
            pltpu.VMEM((hs, LANES), f32),
            pltpu.VMEM((n_rep, rows, depth), bf),
            pltpu.VMEM((pairs, 2, rows, cw), bf),
            pltpu.VMEM((pairs, 2, rows, cw), bf),
            pltpu.VMEM((pairs, 2, rows, cw), bf),
            pltpu.VMEM((n_rep // 2, rows, cw), bf),
            pltpu.VMEM((batch, steps, own_w), bf),
            pltpu.VMEM((1, LANES), f32),
            pltpu.VMEM((n_tp, LANES), f32),
            pltpu.SemaphoreType.DMA((LOADS + 2 * batch + SINGLES + 3 * pairs,)),
            pltpu.SemaphoreType.REGULAR,
        ],
        compiler_params=pltpu.CompilerParams(collective_id=0, has_side_effects=True),
    )(lengths, q, nk, nv, kc, vc, out_weight, stream_in, norm_gain.reshape(own_w // 128, 128))
    return (hidden.astype(bf), (hidden * scale).astype(bf))


def solution(mesh):
    return jax.shard_map(
        functools.partial(on_device, mesh.shape["rep"], mesh.shape["tp"]),
        mesh=mesh,
        in_specs=(
            P("rep", None, "tp"),
            P("rep", None, None),
            P("rep", None, None, None),
            P("rep", None, None, None),
            P("rep", "tp", None, None),
            P("rep", "tp", None, None),
            P("rep"),
            P("tp", "rep"),
            P("tp"),
        ),
        out_specs=(P("rep", None, "tp"), P("rep", None, "tp")),
        check_vma=False,
    )
```

```python
import functools
import math

import jax
import jax.numpy as jnp
from jax import lax
from jax.experimental import pallas as pl
from jax.experimental.pallas import tpu as pltpu
from jax.sharding import PartitionSpec as P

MESH = pl.DeviceIdType.MESH
PAD = 128
LANES = 128
LEAD = 1
TILE = 8
LOADS = 5
SINGLES = 10


def flip(index, mask, count):
    other = 0
    bit = 1
    while bit < count:
        digit = (index // bit) % 2
        other = other + bit * ((1 - digit) if mask & bit else digit)
        bit *= 2
    return other


def landed(ref, sem):
    pltpu.make_async_copy(ref, ref, sem).wait()


def lanes_of(cfg):
    n_rep, n_tp, batch, steps, heads, kv, block_len, width_all, eps = cfg
    group = steps * (heads // kv)
    lane = lax.broadcasted_iota(jnp.int32, (group, LANES), 1)
    row = lax.broadcasted_iota(jnp.int32, (group, LANES), 0)
    return group, lane, row, lane % kv, lane // kv


def score(cfg, b, length, tp, q_v, kv_v):
    n_rep, n_tp, batch, steps, heads, kv, block_len, width_all, eps = cfg
    group, lane, row, kind, place = lanes_of(cfg)
    chunks = block_len * kv // LANES
    causal = (place <= row % steps) & (lane < steps * kv) & (tp == 0)
    s = lax.dot_general(
        q_v[b], kv_v[b, 0], (((1,), (1,)), ((), ())), preferred_element_type=jnp.float32
    )
    left = length - tp * block_len
    kept = []
    for c in range(chunks + 1):
        own = s[0:group, c * LANES : (c + 1) * LANES]
        for g in range(1, kv):
            own = jnp.where(kind == g, s[g * group : (g + 1) * group, c * LANES : (c + 1) * LANES], own)
        seen = place < left - c * (LANES // kv) if c < chunks else causal
        kept.append(jnp.where(seen, own, -1e30))
    return kept


def soften(cfg, kept, scaling):
    kv = cfg[5]
    group, lane, row, kind, place = lanes_of(cfg)
    highest = functools.reduce(jnp.maximum, kept)
    tops = [jnp.max(jnp.where(kind == g, highest, -3e38), axis=1, keepdims=True) for g in range(kv)]
    top = jnp.broadcast_to(tops[0], (group, LANES))
    for g in range(1, kv):
        top = jnp.where(kind == g, tops[g], top)
    weights = [jnp.exp((k - top) * scaling) for k in kept]
    summed = functools.reduce(jnp.add, weights)
    totals = [jnp.sum(jnp.where(kind == g, summed, 0.0), axis=1, keepdims=True) for g in range(kv)]
    rounded = [w.astype(jnp.bfloat16) for w in weights]
    return rounded, jnp.concatenate(tops, axis=0), jnp.concatenate(totals, axis=0)


def blend(cfg, rounded, values):
    kv = cfg[5]
    group, lane, row, kind, place = lanes_of(cfg)
    spread = []
    for g in range(kv):
        one = jnp.where(kind == g, 1.0, 0.0).astype(jnp.bfloat16)
        spread.append(jnp.concatenate([w * one for w in rounded], axis=1))
    spread = jnp.concatenate(spread, axis=0)
    return jnp.dot(spread, values, preferred_element_type=jnp.float32)


def kernel(
    cfg, order, far,
    len_hbm, q_hbm, nk_hbm, nv_hbm, k_hbm, v_hbm, w_hbm, x_hbm, gain_hbm,
    hidden_ref, scale_ref,
    len_s, q_v, kv_v, w_v, gain_v,
    send_o, recv_o, send_l, recv_l, mix,
    gathered, parts, other, ready, recv_c, x_v, sq_s, sq_r,
    sems, news,
):
    n_rep, n_tp, batch, steps, heads, kv, block_len, width_all, eps = cfg
    rep = lax.axis_index("rep")
    tp = lax.axis_index("tp")
    k_own = n_rep // n_tp
    pairs = n_rep // 2
    rows = batch * steps
    owned = heads // n_tp
    orow = owned * steps
    hs = heads * steps
    cached = block_len * kv
    fresh = steps * kv
    cw = w_v.shape[1]
    hd = q_v.shape[2]
    owner = rep // k_own
    core = lax.rem(tp, 2)
    chips = n_tp // 2
    line = rep // 2
    half = pairs // 2
    is_own = (owner == tp) & (core == 0)
    not_own = jnp.logical_not(is_own)
    slot = lax.rem(rep, k_own) * chips + tp // 2

    s_len, s_q, s_w, s_gain, s_x = (sems.at[i] for i in range(LOADS))
    s_kv = [sems.at[LOADS + b] for b in range(batch)]
    s_v = sems.at[LOADS + batch]
    first = LOADS + batch + 1
    (ao_s, ao_r, al_s, al_r, b_s, d_s, c_s, c_r, q_s, q_r) = (
        sems.at[first + i] for i in range(SINGLES)
    )
    first += SINGLES
    b_r = [sems.at[first + p] for p in range(pairs)]
    d_r = [sems.at[first + pairs + p] for p in range(pairs)]
    z_r = [sems.at[first + 2 * pairs + p] for p in range(pairs)]

    loads = [pltpu.make_async_copy(q_hbm, q_v, s_q)]
    for b in range(batch):
        loads += [
            pltpu.make_async_copy(k_hbm.at[b], kv_v.at[b, 0, pl.ds(0, cached)], s_kv[b]),
            pltpu.make_async_copy(nk_hbm.at[b], kv_v.at[b, 0, pl.ds(cached, fresh)], s_kv[b]),
        ]
    loads += [
        pltpu.make_async_copy(len_hbm, len_s, s_len),
        pltpu.make_async_copy(v_hbm, kv_v.at[:, 1, pl.ds(0, cached)], s_v),
        pltpu.make_async_copy(nv_hbm, kv_v.at[:, 1, pl.ds(cached, fresh)], s_v),
    ]
    loads += [
        pltpu.make_async_copy(w_hbm, w_v, s_w),
        pltpu.make_async_copy(gain_hbm, gain_v, s_gain),
        pltpu.make_async_copy(x_hbm, x_v, s_x),
    ]
    for c in loads:
        c.start()

    barrier = pltpu.get_barrier_semaphore()
    leads = tp == LEAD

    def greet(group):
        pl.semaphore_signal(barrier, inc=1, device_id=(group, LEAD), device_id_type=MESH)

    for j in range(n_rep - 1, 0, -1):
        greet(lax.rem(rep + j, n_rep))

    @pl.when(jnp.logical_not(leads))
    def _():
        greet(rep)

    for j in range(1, n_tp):
        peer = lax.rem(tp + j, n_tp)

        @pl.when(peer != LEAD)
        def _():
            pl.semaphore_signal(barrier, inc=1, device_id=(rep, peer), device_id_type=MESH)

    for b in range(batch):
        for i in range(2):
            kv_v[b, i, cached + fresh : cached + PAD, :] = jnp.zeros((PAD - fresh, hd), jnp.bfloat16)

    lane = lax.broadcasted_iota(jnp.int32, (hs, LANES), 1)
    lse = jnp.zeros((hs, LANES), jnp.float32)
    landed(len_s, s_len)
    landed(q_v, s_q)
    scaling = 1.0 / math.sqrt(hd)
    together = batch
    for b0 in range(0, batch, together):
        span = range(b0, b0 + together)
        kept = []
        for b in span:
            landed(kv_v.at[b, 0, pl.ds(0, cached + fresh)], s_kv[b])
            kept.append(score(cfg, b, len_s[b], tp, q_v, kv_v))
        soft = [soften(cfg, k, scaling) for k in kept]
        landed(kv_v.at[:, 1, pl.ds(0, cached + fresh)], s_v)
        if b0 == 0:
            @pl.when(jnp.logical_not(leads))
            def _():
                pl.semaphore_wait(barrier, n_tp - 1)
                pl.semaphore_signal(news, inc=1, device_id=(rep, LEAD), device_id_type=MESH)
        nums = [blend(cfg, soft[i][0], kv_v[b, 1]) for i, b in enumerate(span)]
        for i, b in enumerate(span):
            rounded, tops, total = soft[i]
            out = (nums[i] / total).astype(jnp.bfloat16)
            for t in range(n_tp):
                send_o[t, b] = out[t * orow : (t + 1) * orow]
            lse = jnp.where(lane == b, tops * scaling + jnp.log(total), lse)
    send_l[...] = lse.T[:TILE]

    @pl.when(leads)
    def _():
        pl.semaphore_wait(news, n_tp - 1)

    for mask in [*range(2, n_tp), 1]:
        peer = flip(tp, mask, n_tp)
        pltpu.make_async_remote_copy(
            send_l, recv_l.at[mask - 1], al_s, al_r, device_id=(rep, peer), device_id_type=MESH).start()
        pltpu.make_async_remote_copy(
            send_o.at[peer], recv_o.at[mask - 1], ao_s, ao_r, device_id=(rep, peer), device_id_type=MESH).start()

    @pl.when(leads)
    def _():
        pl.semaphore_wait(barrier, n_rep * n_tp - 1)
        for j in range(1, n_tp):
            pl.semaphore_signal(news, inc=1, device_id=(rep, lax.rem(tp + j, n_tp)), device_id_type=MESH)

    landed(recv_l, al_r)
    ls = [send_l[...]] + [recv_l[j] for j in range(n_tp - 1)]
    most = functools.reduce(jnp.maximum, ls)
    ws = [jnp.exp(l - most) for l in ls]
    inv = 1.0 / functools.reduce(jnp.add, ws)
    ws = [w * inv for w in ws]
    if n_tp * TILE < LANES:
        ws.append(jnp.zeros((LANES - n_tp * TILE, hs), jnp.float32))
    mix[...] = jnp.concatenate(ws, axis=0).T
    share = mix[pl.ds(pl.multiple_of(tp * orow, orow), orow), :]
    landed(recv_o, ao_r)
    att = []
    for b in range(batch):
        acc = share[:, b : b + 1] * send_o[tp, b].astype(jnp.float32)
        for j in range(1, n_tp):
            acc = acc + share[:, j * TILE + b : j * TILE + b + 1] * recv_o[j - 1, b].astype(jnp.float32)
        att.append(acc.astype(jnp.bfloat16))
    att = jnp.concatenate(att, axis=0)
    m = batch * orow
    to = lax.broadcasted_iota(jnp.int32, (m, m), 0)
    frm = lax.broadcasted_iota(jnp.int32, (m, m), 1)
    want = ((to // steps) % batch) * orow + (to // rows) * steps + to % steps
    pick = jnp.where(frm == want, 1.0, 0.0).astype(jnp.bfloat16)
    att = jnp.dot(pick, att, preferred_element_type=jnp.float32).astype(jnp.bfloat16)
    gathered[rep] = jnp.concatenate([att[h * rows : (h + 1) * rows] for h in range(owned)], axis=1)

    @pl.when(jnp.logical_not(leads))
    def _():
        pl.semaphore_wait(news, 1)

    side = lax.rem(rep, 2)
    across = 2 * line + 1 - side
    relays = core == 1
    end = half // 2

    def share(source, target, sem):
        pltpu.make_async_remote_copy(
            gathered.at[source], gathered.at[source], b_s, sem,
            device_id=(target, tp), device_id_type=MESH).start()

    def relay(p):
        landed(gathered.at[p], z_r[p])
        share(2 * p + side, across, b_r[p])

    for mask in far:
        there = flip(line, mask, pairs)
        share(rep, 2 * there + side, sems.at[first + 2 * pairs + line])
        if mask < half:
            share(rep, 2 * there + 1 - side, sems.at[first + line])
        else:
            @pl.when(jnp.logical_not(relays & (line >= half) & (there < end)))
            def _():
                share(rep, 2 * there + 1 - side, sems.at[first + line])

    share(rep, across, sems.at[first + line])

    partner = tp + 1 - 2 * core

    def keeper(p):
        return ((line < half) if p >= half else (line >= half)).astype(jnp.int32)

    def pass_on(p, when):
        @pl.when(when & (core == keeper(p)))
        def _():
            landed(other.at[p], d_r[p])
            for i in range(2):
                both = parts[p, i].astype(jnp.float32) + other[p, i].astype(jnp.float32)
                ready[p, i] = both.astype(jnp.bfloat16)
                local = is_own & (rep == 2 * p + i)

                @pl.when(jnp.logical_not(local))
                def _():
                    pltpu.make_async_remote_copy(
                        ready.at[p, i], recv_c.at[slot], c_s, c_r,
                        device_id=(2 * p + i, owner), device_id_type=MESH).start()

                @pl.when(local)
                def _():
                    recv_c[slot] = ready[p, i]

    landed(w_v, s_w)
    waiting = []
    for batch_of in order:
        distant = functools.reduce(jnp.logical_or, [jnp.abs(line - p) > 1 for p in batch_of])
        for p in waiting:
            pass_on(p, distant)
        for p in batch_of:
            if p == pairs - 1:
                @pl.when(relays & (line < end))
                def _():
                    for q in range(pairs - 1, half - 1, -1):
                        relay(q)

            passed = line == p
            if p >= half:
                passed = passed | (relays & (line < end))

            @pl.when(jnp.logical_not(passed))
            def _():
                landed(gathered.at[2 * p], z_r[p])

            landed(gathered.at[2 * p], b_r[p])

        block = jnp.concatenate([gathered[2 * p + i] for p in batch_of for i in range(2)], axis=0)
        proj = jnp.dot(block, w_v[...], preferred_element_type=jnp.float32).astype(jnp.bfloat16)
        for n, p in enumerate(batch_of):
            for i in range(2):
                parts[p, i] = proj[(2 * n + i) * rows : (2 * n + i + 1) * rows]
            @pl.when(core != keeper(p))
            def _():
                pltpu.make_async_remote_copy(
                    parts.at[p], other.at[p], d_s, d_r[p],
                    device_id=(rep, partner), device_id_type=MESH).start()

        for p in waiting:
            pass_on(p, jnp.logical_not(distant))
        waiting = batch_of
    for p in waiting:
        pass_on(p, line >= 0)

    landed(x_v, s_x)
    landed(gain_v, s_gain)
    gain = gain_v[...].astype(jnp.float32)
    gain = jnp.concatenate([gain[c : c + 1] for c in range(gain.shape[0])], axis=1)

    x = x_v[...].astype(jnp.float32).reshape(rows, x_v.shape[2])
    spot = lax.broadcasted_iota(jnp.int32, (rows, LANES), 0) == lax.broadcasted_iota(jnp.int32, (rows, LANES), 1)

    @pl.when(is_own)
    def _():
        landed(recv_c.at[pl.ds(0, n_rep // 2 - 1)], c_r)

    @pl.when(not_own)
    def _():
        landed(recv_c, c_r)

    pieces = []
    for i in range(k_own):
        acc = recv_c[i * chips].astype(jnp.float32)
        for h in range(1, chips):
            acc = acc + recv_c[i * chips + h].astype(jnp.float32)
        pieces.append(acc)
    hidden = x + jnp.concatenate(pieces, axis=1)
    squares = jnp.sum(hidden * hidden, axis=1, keepdims=True)
    sq_s[...] = jnp.sum(jnp.where(spot, squares, 0.0), axis=0, keepdims=True)
    for mask in [*range(2, n_tp), 1]:
        pltpu.make_async_remote_copy(
            sq_s, sq_r.at[pl.ds(mask, 1)], q_s, q_r,
            device_id=(rep, flip(tp, mask, n_tp)), device_id_type=MESH).start()
    sq_r[0:1, :] = sq_s[...]
    hidden_ref[...] = hidden.reshape(hidden_ref.shape)
    landed(sq_r.at[pl.ds(1, n_tp - 1)], q_r)
    every = jnp.sum(sq_r[...], axis=0, keepdims=True)
    every = jnp.sum(jnp.where(spot, every, 0.0), axis=1, keepdims=True)
    inverse = lax.rsqrt(every / width_all + eps)
    scale_ref[...] = (inverse * gain).reshape(scale_ref.shape)

    landed(recv_l, al_s)
    landed(recv_o, ao_s)
    landed(gathered.at[pl.ds(0, n_rep - 1 - end)], b_s)

    @pl.when(jnp.logical_not(relays & (line >= half)))
    def _():
        landed(gathered.at[pl.ds(0, end)], b_s)

    @pl.when(relays & (line < end))
    def _():
        landed(gathered.at[pl.ds(0, half)], b_s)

    landed(other.at[pl.ds(0, half)], d_s)
    landed(sq_r.at[pl.ds(1, n_tp - 1)], q_s)

    @pl.when(is_own)
    def _():
        landed(recv_c.at[pl.ds(0, n_rep // 2 - 1)], c_s)

    @pl.when(not_own)
    def _():
        landed(recv_c, c_s)


def on_device(
    n_rep, n_tp,
    stream_in, queries, new_keys, new_values, key_cache, value_cache, lengths, out_weight, norm_gain
):
    batch, steps, width = queries.shape
    block_len, kv, hd = key_cache.shape[1:]
    heads = width // hd
    depth, cw = out_weight.shape
    own_w = stream_in.shape[2]
    rows = batch * steps
    k_own = n_rep // n_tp
    assert n_rep & (n_rep - 1) == 0 and n_tp & (n_tp - 1) == 0
    assert n_rep % n_tp == 0 and k_own % 2 == 0 and n_tp % 2 == 0 and heads % n_tp == 0
    assert batch <= TILE and k_own <= TILE and rows <= LANES and n_tp * TILE <= LANES
    owned = heads // n_tp
    orow = owned * steps
    hs = heads * steps
    cached = block_len * kv
    assert cached % LANES == 0 and LANES % kv == 0 and steps * kv <= PAD and hs % LANES == 0
    q = queries.reshape(batch, steps, heads, hd).transpose(0, 2, 1, 3).reshape(batch, hs, hd)
    nk = new_keys.reshape(batch, steps * kv, hd)
    nv = new_values.reshape(batch, steps * kv, hd)
    kc = key_cache.reshape(batch, cached, hd)
    vc = value_cache.reshape(batch, cached, hd)
    cfg = (n_rep, n_tp, batch, steps, heads, kv, block_len, own_w * n_tp, 1e-6)
    pairs = n_rep // 2
    half = pairs // 2
    order = [[0], [1], [3, 2]] if pairs == 4 else [[p] for p in [*range(half), *range(pairs - 1, half - 1, -1)]]
    far = [*range(pairs - 1, 0, -1)]
    bf, f32 = jnp.bfloat16, jnp.float32
    anyspec = pl.BlockSpec(memory_space=pl.ANY)
    vmem = pl.BlockSpec(memory_space=pltpu.VMEM)
    hidden, scale = pl.pallas_call(
        functools.partial(kernel, cfg, order, far),
        out_shape=(
            pltpu.VMEM(stream_in.shape, f32),
            pltpu.VMEM(stream_in.shape, f32),
        ),
        in_specs=[anyspec] * 9,
        out_specs=(vmem, vmem),
        scratch_shapes=[
            pltpu.SMEM((batch,), jnp.int32),
            pltpu.VMEM((batch, hs, hd), bf),
            pltpu.VMEM((batch, 2, cached + PAD, hd), bf),
            pltpu.VMEM((depth, cw), bf),
            pltpu.VMEM((own_w // 128, 128), bf),
            pltpu.VMEM((n_tp, batch, orow, hd), bf),
            pltpu.VMEM((n_tp - 1, batch, orow, hd), bf),
            pltpu.VMEM((TILE, hs), f32),
            pltpu.VMEM((n_tp - 1, TILE, hs), f32),
            pltpu.VMEM((hs, LANES), f32),
            pltpu.VMEM((n_rep, rows, depth), bf),
            pltpu.VMEM((pairs, 2, rows, cw), bf),
            pltpu.VMEM((pairs, 2, rows, cw), bf),
            pltpu.VMEM((pairs, 2, rows, cw), bf),
            pltpu.VMEM((n_rep // 2, rows, cw), bf),
            pltpu.VMEM((batch, steps, own_w), bf),
            pltpu.VMEM((1, LANES), f32),
            pltpu.VMEM((n_tp, LANES), f32),
            pltpu.SemaphoreType.DMA((LOADS + batch + 1 + SINGLES + 3 * pairs,)),
            pltpu.SemaphoreType.REGULAR,
        ],
        compiler_params=pltpu.CompilerParams(collective_id=0, has_side_effects=True),
    )(lengths, q, nk, nv, kc, vc, out_weight, stream_in, norm_gain.reshape(own_w // 128, 128))
    return (hidden.astype(bf), (hidden * scale).astype(bf))


def solution(mesh):
    return jax.shard_map(
        functools.partial(on_device, mesh.shape["rep"], mesh.shape["tp"]),
        mesh=mesh,
        in_specs=(
            P("rep", None, "tp"),
            P("rep", None, None),
            P("rep", None, None, None),
            P("rep", None, None, None),
            P("rep", "tp", None, None),
            P("rep", "tp", None, None),
            P("rep"),
            P("tp", "rep"),
            P("tp"),
        ),
        out_specs=(P("rep", None, "tp"), P("rep", None, "tp")),
        check_vma=False,
    )
```
